32 devices in a mesh: blk: 8 (over y, x, core), lvl: 4 (over z).
Axes of the slice: x: 2, y: 2, z: 4, core: 2. Of those that a mesh axis runs over, the one named last changes fastest.
Arguments:
- vorticity: bfloat16 [4, 3, 64, 32768], P('lvl', None, 'blk'), may hold values from -6 to 6
- shift_field: bfloat16 [4, 64, 32768], P('lvl', 'blk'), may hold values from -0.8984375 to 0.8984375
- new_index: int32 [4, 64], P('lvl', 'blk'), may hold values from 0 to 63, as said below
- parent_slot: int32 [4, 64], P('lvl', 'blk'), may hold values from 0 to 511, as said below
- flags: int32 [4, 64], P('lvl', 'blk'), may hold values 0 or 1
Outputs:
- field: bfloat16 [4, 3, 64, 32768], P('lvl', None, 'blk')
The draws below stay inside these ranges and needn't reach their ends.
Inputs may be any that keep to these rules, and one draw needn't show every extreme that they name: `new_index`: in each level a permutation of the block positions; position b lies on device b // 8 of blk. No device sends more than 2 of its blocks to one device, and that number is reached. `parent_slot`: in each level all values differ; value // 8 is a block of the next coarser level and lies on device value // 64. No device has more than 2 blocks whose parents lie on one device, counting the blocks it holds before migration or those it holds after, and that number is reached in both. The values of level 0 are not used.
All inputs are finite; a program needn't handle non-finite values. No bound on the sum of `flags` on one device may be relied on, other than what follows from the above.
Results may differ from the reference program's by a relative error of at most 0.001.
Values may be sent and summed in bfloat16 or wider, within the bound.
A program may use at most 128 MiB of HBM per device.

```python
import jax
import jax.numpy as jnp

EDGE = 32
CELLS = 32768
B_DEV = 8
CAP = 2
BLOCKS = 64
N_BLK = 8
N_LVL = 4


def joint_routes(key):
    new_levels = []
    parent_levels = []
    for level in range(N_LVL):
        level_key = jax.random.fold_in(key, level)
        placing = jax.random.permutation(jax.random.fold_in(level_key, 1), N_BLK)
        inverse = jnp.zeros((N_BLK,), jnp.int32).at[placing].set(jnp.arange(N_BLK, dtype=jnp.int32))
        offsets = jax.random.permutation(jax.random.fold_in(level_key, 2), N_BLK)[:B_DEV // CAP]
        device_keys = jax.random.split(jax.random.fold_in(level_key, 3), N_BLK)
        shuffle = jax.vmap(lambda one: jax.random.permutation(one, B_DEV))(device_keys)
        groups = offsets[shuffle // CAP]
        target = (inverse[:, None] + groups) % N_BLK
        owners = placing[target]
        new_pos = (owners * B_DEV + shuffle).reshape(BLOCKS).astype(jnp.int32)
        parent_place = jax.random.permutation(jax.random.fold_in(level_key, 4), N_BLK)
        parent_dev = parent_place[(2 * inverse[:, None] + groups) % N_BLK].reshape(BLOCKS).astype(jnp.int32)
        onehot = (parent_dev[:, None] == jnp.arange(N_BLK, dtype=jnp.int32)[None, :]).astype(jnp.int32)
        rank = jnp.sum((jnp.cumsum(onehot, axis=0) - onehot) * onehot, axis=1).astype(jnp.int32)
        slot_keys = jax.random.split(jax.random.fold_in(level_key, 5), N_BLK)
        slots = jax.vmap(lambda one: jax.random.permutation(one, 8 * B_DEV))(slot_keys).astype(jnp.int32)
        value = parent_dev * (8 * B_DEV) + slots[parent_dev, rank]
        parent_at_new = jnp.zeros((BLOCKS,), jnp.int32).at[new_pos].set(value.astype(jnp.int32))
        new_levels.append(new_pos)
        parent_levels.append(parent_at_new)
    return (jnp.stack(new_levels, axis=0).astype(jnp.int32), jnp.stack(parent_levels, axis=0).astype(jnp.int32))


def draw_new_index(key, part):
    return joint_routes(jax.random.fold_in(key, 11))[0]


def draw_parent_slot(key, part):
    return joint_routes(jax.random.fold_in(key, 11))[1]


def set_ends(entries, stream_key, low, largest):
    longest = entries.shape.index(max(entries.shape))
    spots = []
    for shift in (0, 1):
        where = [jax.random.randint(jax.random.fold_in(stream_key, axis), (), 0, length) for axis, length in enumerate(entries.shape)]
        where[longest] = (where[longest] + shift) % entries.shape[longest]
        spots.append(tuple(where))
    return entries.at[spots[0]].set(low).at[spots[1]].set(largest)


def block_levels(rng, dims, cuts, least, top_value):
    loudness = 1.0
    for axis_at, shards_of in cuts:
        steps = jax.random.uniform(jax.random.fold_in(jax.random.fold_in(rng, 6), axis_at), (shards_of,), jnp.float32, least / len(cuts), top_value / len(cuts))
        loudness = loudness * jnp.repeat(jnp.exp(steps), dims[axis_at] // shards_of).reshape((-1,) + (1,) * (len(dims) - 1 - axis_at))
    return loudness


def centred(own_key, extent, width, most, shards=(), kind=jnp.bfloat16):
    factor_of = block_levels(own_key, extent, shards, -0.22, 0.18) if shards else 1.0
    array = jax.random.normal(own_key, extent, jnp.float32) * width * factor_of
    return jnp.minimum(jnp.maximum(array, -most), most).astype(kind)


def setup_inputs(seed: int = 0) -> dict:
    splits = jax.random.split(jax.random.key(seed), 6)
    return {
        "vorticity": centred(splits[0], (N_LVL, 3, BLOCKS, CELLS), 1.0, 6.0, ((0, 4), (2, 8))),
        "shift_field": jnp.clip(jax.random.uniform(splits[1], (N_LVL, BLOCKS, CELLS), jnp.float32, -0.8984375, 0.8984375) * block_levels(splits[1], (N_LVL, BLOCKS, CELLS), ((0, 4), (1, 8)), -0.4, 0.0), -0.8984375, 0.8984375).astype(jnp.bfloat16),
        "new_index": draw_new_index(jax.random.fold_in(splits[5], 71), 0),
        "parent_slot": draw_parent_slot(jax.random.fold_in(splits[5], 71), 0),
        "flags": set_ends((jax.random.randint(splits[4], (N_LVL, BLOCKS), 0, 2) < 1).astype(jnp.int32), jax.random.fold_in(splits[4], 1), 0, 1),
    }


def kernel_weight(distance):
    size = jnp.abs(distance)
    inner = 1.0 - 2.5 * size * size + 1.5 * size * size * size
    outer = 0.5 * (2.0 - size) * (2.0 - size) * (1.0 - size)
    return jnp.where(size < 1.0, inner, jnp.where(size < 2.0, outer, 0.0))


def deposit(values, shifts):
    total = None
    for offset in range(-2, 3):
        weight = kernel_weight(offset - shifts)
        term = values * weight[None]
        padded = jnp.pad(term, ((0, 0), (2 + offset, 2 - offset), (0, 0)))
        total = padded if total is None else total + padded
    return total


def assemble(coarse, marks, count):
    half = EDGE // 2
    full = coarse.reshape(3, count, 2, 2, 2, half, half, half)
    full = full.transpose(0, 1, 2, 5, 3, 6, 4, 7).reshape(3, count, CELLS)
    spread = marks.reshape(count, 2, 2, 2)[:, :, None, :, None, :, None]
    spread = jnp.broadcast_to(spread, (count, 2, half, 2, half, 2, half)).reshape(count, CELLS)
    return full, spread


def reference(vorticity, shift_field, new_index, parent_slot, flags):
    plane = EDGE * EDGE
    length = BLOCKS * EDGE
    half = EDGE // 2
    moved = []
    shrunk = []
    for level in range(N_LVL):
        chain_vort = vorticity[level].astype(jnp.float32).reshape(3, length, plane)
        chain_shift = shift_field[level].astype(jnp.float32).reshape(length, plane)
        remeshed = deposit(chain_vort, chain_shift)[:, 2:length + 2]
        remeshed = remeshed.astype(jnp.bfloat16).reshape(3, BLOCKS, CELLS)
        migrated = jnp.zeros_like(remeshed).at[:, new_index[level]].set(remeshed)
        moved.append(migrated)
        fine = migrated.astype(jnp.float32).reshape(3, BLOCKS, half, 2, half, 2, half, 2)
        shrunk.append((jnp.sum(fine, axis=(3, 5, 7)) * 0.125).reshape(3, BLOCKS, half * half * half))
    results = []
    for level in range(N_LVL):
        base = moved[level].astype(jnp.float32)
        if level + 1 < N_LVL:
            spots = jnp.where(flags[level + 1] == 1, parent_slot[level + 1], 8 * BLOCKS).astype(jnp.int32)
            coarse = jnp.zeros((3, 8 * BLOCKS + 1, half * half * half), jnp.float32)
            coarse = coarse.at[:, spots].set(shrunk[level + 1])[:, :8 * BLOCKS]
            marks = jnp.zeros((8 * BLOCKS + 1,), jnp.float32).at[spots].set(1.0)[:8 * BLOCKS]
            full, spread = assemble(coarse, marks, BLOCKS)
            base = jnp.where(spread[None] > 0.5, full, base)
        results.append(base.astype(jnp.bfloat16))
    return jnp.stack(results, axis=0)
```

```python
import functools

import jax
import jax.numpy as jnp
import numpy as np
from jax import lax
from jax.experimental import pallas as pl
from jax.experimental.pallas import tpu as pltpu
from jax.sharding import PartitionSpec as P

MESH = pl.DeviceIdType.MESH
EDGE = 32
PLANE = EDGE * EDGE
HALO = 2 * PLANE
CAP = 2
VMEM_LIMIT = 60 * 1024 * 1024


def device(blk, lvl):
    return {"blk": blk, "lvl": lvl}


def enter(n, levels, me, lvl):
    barrier = pltpu.get_barrier_semaphore()

    def greet(blk, level):
        pl.semaphore_signal(barrier, inc=1, device_id=device(blk, level), device_id_type=MESH)

    for k in range(1, n):
        greet(lax.rem(me + k, n), lvl)

    @pl.when(lvl > 0)
    def _():
        for k in range(n):
            greet(lax.rem(me + k, n), lvl - 1)

    @pl.when(lvl < levels - 1)
    def _():
        for k in range(n):
            greet(lax.rem(me + k, n), lvl + 1)

    pl.semaphore_wait(
        barrier, n - 1 + n * ((lvl > 0).astype(jnp.int32) + (lvl < levels - 1).astype(jnp.int32))
    )


def remote(src, dst, send, recv, target):
    return pltpu.make_async_remote_copy(
        src_ref=src, dst_ref=dst, send_sem=send, recv_sem=recv, device_id=target, device_id_type=MESH
    )


def share_kernel(n, levels, tab, vort, shift, below_v, below_s, above_v, above_s, tables,
                 near_s, near_r, coarse_s, coarse_r, halo_s, halo_r):
    me = lax.axis_index("blk")
    lvl = lax.axis_index("lvl")
    cells = vort.shape[2]
    enter(n, levels, me, lvl)

    def high(target):
        part = pl.ds(cells - HALO, HALO)
        return (
            remote(vort.at[:, :, part], below_v, halo_s.at[0], halo_r.at[0], target),
            remote(shift.at[:, part], below_s, halo_s.at[1], halo_r.at[1], target),
        )

    def low(target):
        part = pl.ds(0, HALO)
        return (
            remote(vort.at[:, :, part], above_v, halo_s.at[2], halo_r.at[2], target),
            remote(shift.at[:, part], above_s, halo_s.at[3], halo_r.at[3], target),
        )

    after = device(lax.rem(me + 1, n), lvl)
    before = device(lax.rem(me + n - 1, n), lvl)

    @pl.when(me < n - 1)
    def _():
        for copy in high(after):
            copy.start()

    @pl.when(me > 0)
    def _():
        for copy in low(before):
            copy.start()

    near = [
        remote(tab, tables.at[0, me], near_s.at[k], near_r.at[k], device(lax.rem(me + k, n), lvl))
        for k in range(1, n)
    ]
    for copy in near:
        copy.start()
    coarse_level = jnp.maximum(lvl - 1, 0)

    @pl.when(lvl > 0)
    def _():
        for k in range(n):
            remote(tab, tables.at[1, me], coarse_s.at[k], coarse_r.at[k],
                   device(lax.rem(me + k, n), coarse_level)).start()

    tables[0, me] = tab[...]
    for k in range(1, n):
        source = lax.rem(me + n - k, n)
        remote(tab, tables.at[0, source], near_s.at[k], near_r.at[k], before).wait_recv()
        near[k - 1].wait_send()

    @pl.when(lvl > 0)
    def _():
        for k in range(n):
            remote(tab, tables.at[1, me], coarse_s.at[k], coarse_r.at[k],
                   device(lax.rem(me + k, n), coarse_level)).wait_send()

    @pl.when(lvl < levels - 1)
    def _():
        for k in range(n):
            source = lax.rem(me + n - k, n)
            remote(tab, tables.at[1, source], coarse_s.at[k], coarse_r.at[k], before).wait_recv()

    @pl.when(me < n - 1)
    def _():
        for copy in high(after):
            copy.wait_send()
        for copy in low(after):
            copy.wait_recv()

    @pl.when(me > 0)
    def _():
        for copy in low(before):
            copy.wait_send()
        for copy in high(before):
            copy.wait_recv()


def tap_weights(shifts):
    size = jnp.abs(shifts)
    rest = 1.0 - size
    size2 = size * size
    rest2 = rest * rest
    middle = 1.0 + size2 * (1.5 * size - 2.5)
    ahead = 1.0 + rest2 * (1.5 * rest - 2.5)
    behind = -0.5 * rest2 * size
    far = -0.5 * size2 * rest
    up = shifts >= 0.0
    return {
        -2: jnp.where(up, 0.0, far),
        -1: jnp.where(up, behind, ahead),
        0: middle,
        1: jnp.where(up, ahead, behind),
        2: jnp.where(up, far, 0.0),
    }


def remesh_kernel(n, tables, vort, shift, below_v, below_s, above_v, above_s, shrink, send, ghost, rows):
    me = lax.axis_index("blk")
    blocks = vort.shape[1]
    lane_tiles = PLANE // 128
    sublane = lax.broadcasted_iota(jnp.int32, (blocks, 128), 0)

    def tile(ref, c, at):
        part = ref[c, :, pl.ds(at, 128)] if c is not None else ref[:, pl.ds(at, 128)]
        return part.astype(jnp.float32)

    def source_tile(own, low, high, c, x, j):
        if 0 <= x < EDGE:
            return tile(own, c, pl.multiple_of(x * PLANE + j * 128, 128))
        if x < 0:
            inner = pltpu.roll(tile(own, c, pl.multiple_of((EDGE + x) * PLANE + j * 128, 128)), 1, 0)
            outer = pltpu.roll(tile(low, c, pl.multiple_of((2 + x) * PLANE + j * 128, 128)), 1, 0)
            outer = jnp.where(me == 0, 0.0, outer)
            return jnp.where(sublane == 0, outer, inner)
        inner = pltpu.roll(tile(own, c, pl.multiple_of((x - EDGE) * PLANE + j * 128, 128)), blocks - 1, 0)
        outer = pltpu.roll(tile(high, c, pl.multiple_of((x - EDGE) * PLANE + j * 128, 128)), blocks - 1, 0)
        outer = jnp.where(me == n - 1, 0.0, outer)
        return jnp.where(sublane == blocks - 1, outer, inner)

    def chunk(j, carry):
        sums = {}
        for x in range(-2, EDGE + 2):
            weights = tap_weights(source_tile(shift, below_s, above_s, None, x, j))
            for c in range(3):
                value = source_tile(vort, below_v, above_v, c, x, j)
                for offset in range(-2, 3):
                    to = x + offset
                    if 0 <= to < EDGE:
                        term = value * weights[offset]
                        sums[to, c] = sums[to, c] + term if (to, c) in sums else term
            done = x - 2
            if 0 <= done < EDGE:
                for c in range(3):
                    at = pl.multiple_of((done * lane_tiles + j) * blocks, blocks)
                    rows[c, pl.ds(at, blocks), :] = sums.pop((done, c))
        return carry

    lax.fori_loop(0, lane_tiles, chunk, 0)

    height = rows.shape[1] // blocks
    quarter = height // 4
    owners, parents = [], []
    for b in range(blocks):
        position = tables[0, me, 0, b]
        home = lax.div(position, blocks)
        parent = tables[0, home, 0, blocks + lax.rem(position, blocks)]
        parent_owner = lax.div(parent, 8 * blocks)
        rank = sum([(home == other).astype(jnp.int32) for other in owners], jnp.int32(0))
        parent_rank = sum([(parent_owner == other).astype(jnp.int32) for other in parents], jnp.int32(0))
        owners.append(home)
        parents.append(parent_owner)
        for c in range(3):
            block = rows[c, pl.ds(b, height, stride=blocks), :].astype(jnp.bfloat16)
            send[home, rank, c] = block
            wide = jnp.concatenate([block[q * quarter:(q + 1) * quarter] for q in range(4)], axis=1)
            pairs = jnp.dot(wide, shrink[...], preferred_element_type=jnp.float32)
            pairs = pairs.reshape(4, 2, 8, 128)
            ghost[parent_owner, parent_rank, c] = (
                (pairs[:, 0] + pairs[:, 1]).reshape(32, 128).astype(jnp.bfloat16)
            )


def exchange_kernel(n, levels, send, ghost, got, got_ghost, near_s, near_r, coarse_s, coarse_r):
    me = lax.axis_index("blk")
    lvl = lax.axis_index("lvl")
    coarse_level = jnp.maximum(lvl - 1, 0)
    enter(n, levels, me, lvl)

    def near(k):
        to = lax.rem(me + k, n)
        return remote(send.at[to], got.at[me], near_s.at[k], near_r.at[k], device(to, lvl))

    def coarse(k):
        to = lax.rem(me + k, n)
        return remote(ghost.at[to], got_ghost.at[me], coarse_s.at[k], coarse_r.at[k],
                      device(to, coarse_level))

    for k in range(1, n):
        near(k).start()

    @pl.when(lvl > 0)
    def _():
        for k in range(n):
            coarse(k).start()

    before = device(lax.rem(me + n - 1, n), lvl)
    for k in range(1, n):
        source = lax.rem(me + n - k, n)
        remote(send.at[me], got.at[source], near_s.at[k], near_r.at[k], before).wait_recv()

    @pl.when(lvl < levels - 1)
    def _():
        for k in range(n):
            source = lax.rem(me + n - k, n)
            remote(ghost.at[me], got_ghost.at[source], coarse_s.at[k], coarse_r.at[k], before).wait_recv()

    for k in range(1, n):
        near(k).wait_send()

    @pl.when(lvl > 0)
    def _():
        for k in range(n):
            coarse(k).wait_send()


def settle_kernel(n, levels, tables, send, got, got_ghost, grow, out, rows):
    me = lax.axis_index("blk")
    lvl = lax.axis_index("lvl")
    blocks = out.shape[1]
    height = rows.shape[1] // blocks

    def place(e, count):
        source = lax.div(e, blocks)
        b = lax.rem(e, blocks)
        count = jnp.where(b == 0, 0, count)
        position = tables[0, source, 0, b]
        mine = lax.div(position, blocks) == me
        spot = lax.rem(position, blocks)

        def put(ref):
            for c in range(3):
                rows[c, pl.ds(spot, height, stride=blocks), :] = ref[source, count, c].astype(jnp.float32)

        @pl.when(jnp.logical_and(mine, source == me))
        def _():
            put(send)

        @pl.when(jnp.logical_and(mine, source != me))
        def _():
            put(got)

        return count + mine.astype(jnp.int32)

    lax.fori_loop(0, n * blocks, place, jnp.int32(0))

    row = lax.broadcasted_iota(jnp.int32, (32, 32), 0)
    column = lax.broadcasted_iota(jnp.int32, (32, 32), 1)
    mask_row = lax.broadcasted_iota(jnp.int32, (32, 128), 0)
    mask_lane = lax.broadcasted_iota(jnp.int32, (32, 128), 1)

    def refine(e, count):
        source = lax.div(e, blocks)
        b = lax.rem(e, blocks)
        count = jnp.where(b == 0, 0, count)
        position = tables[1, source, 0, b]
        home = lax.div(position, blocks)
        local = lax.rem(position, blocks)
        parent = tables[1, home, 0, blocks + local]
        flag = tables[1, home, 0, 2 * blocks + local]
        mine = lax.div(parent, 8 * blocks) == me

        @pl.when(jnp.logical_and(mine, flag == 1))
        def _():
            code = lax.rem(parent, 8 * blocks)
            spot = lax.div(code, 8)
            ox = lax.rem(lax.div(code, 4), 2)
            oy = lax.rem(lax.div(code, 2), 2)
            oz = lax.rem(code, 2)
            spread = []
            for half in range(2):
                hot = jnp.logical_and(row // 8 == column // 8,
                                      column % 8 == 2 * (row % 8 - 4 * oy) + half)
                spread.append(hot.astype(jnp.float32).astype(jnp.bfloat16))
            mask = jnp.logical_and(mask_row % 8 // 4 == oy, mask_lane % 32 // 16 == oz)
            for c in range(3):
                block = got_ghost[source, count, c]
                wide = jnp.concatenate(
                    [jnp.dot(part, block, preferred_element_type=jnp.float32) for part in spread], axis=1
                ).astype(jnp.bfloat16)
                full = jnp.dot(wide, grow[oz], preferred_element_type=jnp.float32)
                for q in range(4):
                    where = pl.ds((ox * 128 + q * 32) * blocks + spot, 32, stride=blocks)
                    rows[c, where, :] = jnp.where(
                        mask, full[:, q * 128:(q + 1) * 128], rows[c, where, :]
                    )

        return count + mine.astype(jnp.int32)

    lax.fori_loop(0, jnp.where(lvl < levels - 1, n * blocks, 0), refine, jnp.int32(0))

    def finish(r, carry):
        for c in range(3):
            for step in range(8):
                at = r * 8 + step
                out[c, :, pl.ds(pl.multiple_of(at * 128, 128), 128)] = rows[
                    c, pl.ds(pl.multiple_of(at * blocks, blocks), blocks), :
                ].astype(jnp.bfloat16)
        return carry

    lax.fori_loop(0, height // 8, finish, 0)


def selection_tables():
    src = np.arange(512)
    to = np.arange(128)
    q, y, z = src // 128, src % 128 // 32, src % 32
    target = q * 32 + (y // 2) * 16 + z // 2
    shrink = np.where(target[:, None] == to[None, :], 0.125, 0.0)
    part = np.arange(256)
    half, pq, py, pz = part // 128, part % 128 // 32, part % 32 // 16, part % 16
    grow = np.zeros((2, 256, 512))
    for oz in range(2):
        grow[oz, part, pq * 128 + (2 * half + py) * 32 + oz * 16 + pz] = 1.0
    return shrink, grow


def body(n, levels, vorticity, shift_field, new_index, parent_slot, flags):
    blocks, cells = vorticity.shape[2:]
    vort, shift = vorticity[0], shift_field[0]
    tab = jnp.concatenate([new_index, parent_slot, flags], axis=1)
    tab = jnp.pad(tab, ((0, 0), (0, 128 - 3 * blocks)))
    any_space = pl.BlockSpec(memory_space=pl.ANY)
    vmem = pl.BlockSpec(memory_space=pltpu.VMEM)
    smem = pl.BlockSpec(memory_space=pltpu.SMEM)
    bf16 = jnp.bfloat16
    shape = jax.ShapeDtypeStruct
    dma = pltpu.SemaphoreType.DMA
    height = cells // 128

    below_v, below_s, above_v, above_s, tables = pl.pallas_call(
        functools.partial(share_kernel, n, levels),
        out_shape=(
            shape((3, blocks, HALO), bf16), shape((blocks, HALO), bf16),
            shape((3, blocks, HALO), bf16), shape((blocks, HALO), bf16),
            shape((2, n, 1, 128), jnp.int32),
        ),
        in_specs=[vmem, any_space, any_space],
        out_specs=(any_space, any_space, any_space, any_space, vmem),
        scratch_shapes=[dma((n,)), dma((n,)), dma((n,)), dma((n,)), dma((4,)), dma((4,))],
        compiler_params=pltpu.CompilerParams(collective_id=0, has_side_effects=True),
        name="share",
    )(tab, vort, shift)

    shrink, grow = selection_tables()
    send, ghost = pl.pallas_call(
        functools.partial(remesh_kernel, n),
        out_shape=(
            shape((n, CAP, 3, height, 128), bf16),
            shape((n, CAP, 3, 32, 128), bf16),
        ),
        in_specs=[smem] + [vmem] * 7,
        out_specs=(vmem, vmem),
        scratch_shapes=[pltpu.VMEM((3, height * blocks, 128), jnp.float32)],
        compiler_params=pltpu.CompilerParams(vmem_limit_bytes=VMEM_LIMIT),
        name="remesh",
    )(tables, vort, shift, below_v, below_s, above_v, above_s, jnp.asarray(shrink, bf16))

    got, got_ghost = pl.pallas_call(
        functools.partial(exchange_kernel, n, levels),
        out_shape=(shape(send.shape, bf16), shape(ghost.shape, bf16)),
        in_specs=[any_space] * 2,
        out_specs=(any_space,) * 2,
        scratch_shapes=[dma((n,)), dma((n,)), dma((n,)), dma((n,))],
        compiler_params=pltpu.CompilerParams(collective_id=1, has_side_effects=True),
        name="exchange",
    )(send, ghost)

    out = pl.pallas_call(
        functools.partial(settle_kernel, n, levels),
        out_shape=shape((3, blocks, cells), bf16),
        in_specs=[smem] + [vmem] * 4,
        out_specs=vmem,
        scratch_shapes=[pltpu.VMEM((3, height * blocks, 128), jnp.float32)],
        compiler_params=pltpu.CompilerParams(vmem_limit_bytes=VMEM_LIMIT),
        name="settle",
    )(tables, send, got, got_ghost, jnp.asarray(grow, bf16))
    return out[None]


def solution(mesh):
    placed = (
        P("lvl", None, "blk", None),
        P("lvl", "blk", None),
        P("lvl", "blk"),
        P("lvl", "blk"),
        P("lvl", "blk"),
    )
    step = functools.partial(body, mesh.shape["blk"], mesh.shape["lvl"])
    return jax.shard_map(
        step, mesh=mesh, in_specs=placed, out_specs=P("lvl", None, "blk", None), check_vma=False
    )
```

```python
import functools

import jax
import jax.numpy as jnp
import numpy as np
from jax import lax
from jax.experimental import pallas as pl
from jax.experimental.pallas import tpu as pltpu
from jax.sharding import PartitionSpec as P

MESH = pl.DeviceIdType.MESH
EDGE = 32
PLANE = EDGE * EDGE
HALO = 2 * PLANE
CAP = 2
VMEM_LIMIT = 60 * 1024 * 1024


def device(blk, lvl):
    return {"blk": blk, "lvl": lvl}


def enter(n, levels, me, lvl):
    barrier = pltpu.get_barrier_semaphore()

    def greet(blk, level):
        pl.semaphore_signal(barrier, inc=1, device_id=device(blk, level), device_id_type=MESH)

    for k in range(1, n):
        greet(lax.rem(me + k, n), lvl)

    @pl.when(lvl > 0)
    def _():
        for k in range(n):
            greet(lax.rem(me + k, n), lvl - 1)

    @pl.when(lvl < levels - 1)
    def _():
        for k in range(n):
            greet(lax.rem(me + k, n), lvl + 1)

    pl.semaphore_wait(
        barrier, n - 1 + n * ((lvl > 0).astype(jnp.int32) + (lvl < levels - 1).astype(jnp.int32))
    )


def remote(src, dst, send, recv, target):
    return pltpu.make_async_remote_copy(
        src_ref=src, dst_ref=dst, send_sem=send, recv_sem=recv, device_id=target, device_id_type=MESH
    )


def tap_weights(shifts):
    size = jnp.abs(shifts)
    rest = 1.0 - size
    size2 = size * size
    rest2 = rest * rest
    middle = 1.0 + size2 * (1.5 * size - 2.5)
    ahead = 1.0 + rest2 * (1.5 * rest - 2.5)
    behind = -0.5 * rest2 * size
    far = -0.5 * size2 * rest
    up = shifts >= 0.0
    return {
        -2: jnp.where(up, 0.0, far),
        -1: jnp.where(up, behind, ahead),
        0: middle,
        1: jnp.where(up, ahead, behind),
        2: jnp.where(up, far, 0.0),
    }


def picks(keys, wanted):
    count, first, second = jnp.int32(0), jnp.int32(0), jnp.int32(0)
    for b, key in enumerate(keys):
        hit = key == wanted
        first = jnp.where(jnp.logical_and(hit, count == 0), b, first)
        second = jnp.where(jnp.logical_and(hit, count == 1), b, second)
        count = count + hit.astype(jnp.int32)
    return first, second


def move_kernel(n, levels, spots, tab, vort, shift, shrink,
                got0, got1, got2, got_ghost, tables,
                send0, send1, send2, ghost, below_v, below_s, above_v, above_s, rows, whole, small, local,
                near_s, near_r, coarse_s, coarse_r, halo_s, halo_r, block_s, block_r, ghost_s, ghost_r,
                own_sem, table_sem):
    me = lax.axis_index("blk")
    lvl = lax.axis_index("lvl")
    blocks, cells = vort.shape[1:]
    lane_tiles = PLANE // 128
    height = cells // 128
    quarter = height // 4
    coarse_level = jnp.maximum(lvl - 1, 0)
    got, send = (got0, got1, got2), (send0, send1, send2)
    after = device(lax.rem(me + 1, n), lvl)
    before = device(lax.rem(me + n - 1, n), lvl)
    enter(n, levels, me, lvl)

    def high(target):
        part = pl.ds(cells - HALO, HALO)
        return (
            remote(vort.at[:, :, part], below_v, halo_s.at[0], halo_r.at[0], target),
            remote(shift.at[:, part], below_s, halo_s.at[1], halo_r.at[1], target),
        )

    def low(target):
        part = pl.ds(0, HALO)
        return (
            remote(vort.at[:, :, part], above_v, halo_s.at[2], halo_r.at[2], target),
            remote(shift.at[:, part], above_s, halo_s.at[3], halo_r.at[3], target),
        )

    def near(k):
        return remote(tab, tables.at[0, me], near_s.at[k], near_r.at[k], device(lax.rem(me + k, n), lvl))

    def coarse(k):
        return remote(tab, tables.at[1, me], coarse_s.at[k], coarse_r.at[k],
                      device(lax.rem(me + k, n), coarse_level))

    @pl.when(me < n - 1)
    def _():
        for copy in high(after):
            copy.start()

    @pl.when(me > 0)
    def _():
        for copy in low(before):
            copy.start()

    for k in range(1, n):
        near(k).start()

    @pl.when(lvl > 0)
    def _():
        for k in range(n):
            coarse(k).start()

    tables[0, me] = tab[...]
    owners = [lax.div(spots[0, b], blocks) for b in range(blocks)]

    @pl.when(me < n - 1)
    def _():
        for copy in low(after):
            copy.wait_recv()

    @pl.when(me > 0)
    def _():
        for copy in high(before):
            copy.wait_recv()

    sublane = lax.broadcasted_iota(jnp.int32, (blocks, 128), 0)

    def tile(ref, c, at):
        part = ref[c, :, pl.ds(at, 128)] if c is not None else ref[:, pl.ds(at, 128)]
        return part.astype(jnp.float32)

    def source_tile(own, below, above, c, x, j):
        if 0 <= x < EDGE:
            return tile(own, c, pl.multiple_of(x * PLANE + j * 128, 128))
        if x < 0:
            inner = pltpu.roll(tile(own, c, pl.multiple_of((EDGE + x) * PLANE + j * 128, 128)), 1, 0)
            outer = pltpu.roll(tile(below, c, pl.multiple_of((2 + x) * PLANE + j * 128, 128)), 1, 0)
            outer = jnp.where(me == 0, 0.0, outer)
            return jnp.where(sublane == 0, outer, inner)
        at = pl.multiple_of((x - EDGE) * PLANE + j * 128, 128)
        inner = pltpu.roll(tile(own, c, at), blocks - 1, 0)
        outer = pltpu.roll(tile(above, c, at), blocks - 1, 0)
        outer = jnp.where(me == n - 1, 0.0, outer)
        return jnp.where(sublane == blocks - 1, outer, inner)

    def remesh(c):
        def chunk(j, carry):
            sums = {}
            for x in range(-2, EDGE + 2):
                weights = tap_weights(source_tile(shift, below_s, above_s, None, x, j))
                value = source_tile(vort, below_v, above_v, c, x, j)
                for offset in range(-2, 3):
                    to = x + offset
                    if 0 <= to < EDGE:
                        term = value * weights[offset]
                        sums[to] = sums[to] + term if to in sums else term
                done = x - 2
                if 0 <= done < EDGE:
                    at = pl.multiple_of((done * lane_tiles + j) * blocks, blocks)
                    rows[pl.ds(at, blocks), :] = sums.pop(done)
            return carry

        lax.fori_loop(0, lane_tiles, chunk, 0)
        for b in range(blocks):
            whole[b] = rows[pl.ds(b, height, stride=blocks), :].astype(jnp.bfloat16)

    def block_copy(c, k):
        to = lax.rem(me + k, n)
        return remote(send[c].at[to], got[c].at[me], block_s.at[c, k], block_r.at[c, k], device(to, lvl))

    def own_copy(c):
        return pltpu.make_async_copy(send[c].at[me], got[c].at[me], own_sem.at[c])

    def ghost_copy(c, k):
        to = lax.rem(me + k, n)
        return remote(ghost.at[c, to], got_ghost.at[c, me], ghost_s.at[c, k], ghost_r.at[c, k],
                      device(to, coarse_level))

    def send_blocks(c):
        def pack(k, carry):
            to = lax.rem(me + k, n)
            first, second = picks(owners, to)
            send[c][to, 0] = whole[first]
            send[c][to, 1] = whole[second]
            return carry

        lax.fori_loop(1, n + 1, pack, 0)
        for k in range(1, n):
            block_copy(c, k).start()
        own_copy(c).start()

    def restrict(c):
        for b in range(blocks):
            block = whole[b]
            wide = jnp.concatenate([block[q * quarter:(q + 1) * quarter] for q in range(4)], axis=1)
            pairs = jnp.dot(wide, shrink[...], preferred_element_type=jnp.float32)
            pairs = pairs.reshape(4, 2, 8, 128)
            small[c, b] = (pairs[:, 0] + pairs[:, 1]).reshape(32, 128).astype(jnp.bfloat16)

    def send_ghosts(c, parents):
        def pack(k, carry):
            to = lax.rem(me + k, n)
            first, second = picks(parents, to)
            ghost[c, to, 0] = small[c, first]
            ghost[c, to, 1] = small[c, second]
            return carry

        lax.fori_loop(0, n, pack, 0)

        @pl.when(lvl > 0)
        def _():
            for k in range(n):
                ghost_copy(c, k).start()

    remesh(0)
    send_blocks(0)

    for k in range(1, n):
        source = lax.rem(me + n - k, n)
        remote(tab, tables.at[0, source], near_s.at[k], near_r.at[k], before).wait_recv()
    fetch = pltpu.make_async_copy(tables.at[0], local, table_sem)
    fetch.start()
    restrict(0)
    fetch.wait()
    parents = []
    for b in range(blocks):
        home, spot = lax.div(spots[0, b], blocks), lax.rem(spots[0, b], blocks)
        parents.append(lax.div(local[home, 0, blocks + spot], 8 * blocks))
    send_ghosts(0, parents)
    remesh(1)
    send_blocks(1)
    restrict(1)
    send_ghosts(1, parents)
    remesh(2)
    restrict(2)
    send_ghosts(2, parents)
    send_blocks(2)

    @pl.when(lvl > 0)
    def _():
        for k in range(n):
            coarse(k).wait_send()
            for c in range(3):
                ghost_copy(c, k).wait_send()

    @pl.when(lvl < levels - 1)
    def _():
        for k in range(n):
            source = lax.rem(me + n - k, n)
            remote(tab, tables.at[1, source], coarse_s.at[k], coarse_r.at[k], before).wait_recv()

    @pl.when(me < n - 1)
    def _():
        for copy in high(after):
            copy.wait_send()

    @pl.when(me > 0)
    def _():
        for copy in low(before):
            copy.wait_send()

    for k in range(1, n):
        near(k).wait_send()
    for c in range(3):
        own_copy(c).wait()
        for k in range(1, n):
            source = lax.rem(me + n - k, n)
            remote(send[c].at[me], got[c].at[source], block_s.at[c, k], block_r.at[c, k], before).wait_recv()
            block_copy(c, k).wait_send()

    @pl.when(lvl < levels - 1)
    def _():
        for c in range(3):
            for k in range(n):
                source = lax.rem(me + n - k, n)
                remote(ghost.at[c, me], got_ghost.at[c, source], ghost_s.at[c, k], ghost_r.at[c, k],
                       before).wait_recv()


def settle_kernel(n, levels, tables, got0, got1, got2, got_ghost, grow, out, rows):
    me = lax.axis_index("blk")
    lvl = lax.axis_index("lvl")
    blocks = out.shape[1]
    height = rows.shape[1] // blocks

    def place(e, count):
        source = lax.div(e, blocks)
        b = lax.rem(e, blocks)
        count = jnp.where(b == 0, 0, count)
        position = tables[0, source, 0, b]
        mine = lax.div(position, blocks) == me
        spot = lax.rem(position, blocks)

        @pl.when(mine)
        def _():
            for c, got in enumerate((got0, got1, got2)):
                rows[c, pl.ds(spot, height, stride=blocks), :] = got[source, count].astype(jnp.float32)

        return count + mine.astype(jnp.int32)

    lax.fori_loop(0, n * blocks, place, jnp.int32(0))

    row = lax.broadcasted_iota(jnp.int32, (32, 32), 0)
    column = lax.broadcasted_iota(jnp.int32, (32, 32), 1)
    mask_row = lax.broadcasted_iota(jnp.int32, (32, 128), 0)
    mask_lane = lax.broadcasted_iota(jnp.int32, (32, 128), 1)

    def refine(e, count):
        source = lax.div(e, blocks)
        b = lax.rem(e, blocks)
        count = jnp.where(b == 0, 0, count)
        position = tables[1, source, 0, b]
        home = lax.div(position, blocks)
        local = lax.rem(position, blocks)
        parent = tables[1, home, 0, blocks + local]
        flag = tables[1, home, 0, 2 * blocks + local]
        mine = lax.div(parent, 8 * blocks) == me

        @pl.when(jnp.logical_and(mine, flag == 1))
        def _():
            code = lax.rem(parent, 8 * blocks)
            spot = lax.div(code, 8)
            ox = lax.rem(lax.div(code, 4), 2)
            oy = lax.rem(lax.div(code, 2), 2)
            oz = lax.rem(code, 2)
            spread = []
            for half in range(2):
                hot = jnp.logical_and(row // 8 == column // 8,
                                      column % 8 == 2 * (row % 8 - 4 * oy) + half)
                spread.append(hot.astype(jnp.float32).astype(jnp.bfloat16))
            mask = jnp.logical_and(mask_row % 8 // 4 == oy, mask_lane % 32 // 16 == oz)
            for c in range(3):
                block = got_ghost[c, source, count]
                wide = jnp.concatenate(
                    [jnp.dot(part, block, preferred_element_type=jnp.float32) for part in spread], axis=1
                ).astype(jnp.bfloat16)
                full = jnp.dot(wide, grow[oz], preferred_element_type=jnp.float32)
                for q in range(4):
                    where = pl.ds((ox * 128 + q * 32) * blocks + spot, 32, stride=blocks)
                    rows[c, where, :] = jnp.where(
                        mask, full[:, q * 128:(q + 1) * 128], rows[c, where, :]
                    )

        return count + mine.astype(jnp.int32)

    lax.fori_loop(0, jnp.where(lvl < levels - 1, n * blocks, 0), refine, jnp.int32(0))

    def finish(r, carry):
        for c in range(3):
            for step in range(8):
                at = r * 8 + step
                out[c, :, pl.ds(pl.multiple_of(at * 128, 128), 128)] = rows[
                    c, pl.ds(pl.multiple_of(at * blocks, blocks), blocks), :
                ].astype(jnp.bfloat16)
        return carry

    lax.fori_loop(0, height // 8, finish, 0)


def selection_tables():
    src = np.arange(512)
    to = np.arange(128)
    q, y, z = src // 128, src % 128 // 32, src % 32
    target = q * 32 + (y // 2) * 16 + z // 2
    shrink = np.where(target[:, None] == to[None, :], 0.125, 0.0)
    part = np.arange(256)
    half, pq, py, pz = part // 128, part % 128 // 32, part % 32 // 16, part % 16
    grow = np.zeros((2, 256, 512))
    for oz in range(2):
        grow[oz, part, pq * 128 + (2 * half + py) * 32 + oz * 16 + pz] = 1.0
    return shrink, grow


def body(n, levels, vorticity, shift_field, new_index, parent_slot, flags):
    blocks, cells = vorticity.shape[2:]
    vort, shift = vorticity[0], shift_field[0]
    tab = jnp.concatenate([new_index, parent_slot, flags], axis=1)
    tab = jnp.pad(tab, ((0, 0), (0, 128 - 3 * blocks)))
    any_space = pl.BlockSpec(memory_space=pl.ANY)
    vmem = pl.BlockSpec(memory_space=pltpu.VMEM)
    smem = pl.BlockSpec(memory_space=pltpu.SMEM)
    bf16 = jnp.bfloat16
    shape = jax.ShapeDtypeStruct
    dma = pltpu.SemaphoreType.DMA
    height = cells // 128

    shrink, grow = selection_tables()
    many = shape((n, CAP, height, 128), bf16)
    vm = pltpu.VMEM
    got0, got1, got2, got_ghost, tables = pl.pallas_call(
        functools.partial(move_kernel, n, levels),
        out_shape=(many, many, many, shape((3, n, CAP, 32, 128), bf16), shape((2, n, 1, 128), jnp.int32)),
        in_specs=[smem, vmem, vmem, vmem, vmem],
        out_specs=(any_space,) * 4 + (vmem,),
        scratch_shapes=[
            vm(many.shape, bf16), vm(many.shape, bf16), vm(many.shape, bf16),
            vm((3, n, CAP, 32, 128), bf16),
            vm((3, blocks, HALO), bf16), vm((blocks, HALO), bf16),
            vm((3, blocks, HALO), bf16), vm((blocks, HALO), bf16),
            vm((height * blocks, 128), jnp.float32), vm((blocks, height, 128), bf16),
            vm((3, blocks, 32, 128), bf16), pltpu.SMEM((n, 1, 128), jnp.int32),
            dma((n,)), dma((n,)), dma((n,)), dma((n,)), dma((4,)), dma((4,)),
            dma((3, n)), dma((3, n)), dma((3, n)), dma((3, n)), dma((3,)), dma,
        ],
        compiler_params=pltpu.CompilerParams(
            collective_id=0, has_side_effects=True, vmem_limit_bytes=VMEM_LIMIT
        ),
        name="move",
    )(new_index, tab, vort, shift, jnp.asarray(shrink, bf16))

    out = pl.pallas_call(
        functools.partial(settle_kernel, n, levels),
        out_shape=shape((3, blocks, cells), bf16),
        in_specs=[smem] + [vmem] * 5,
        out_specs=vmem,
        scratch_shapes=[pltpu.VMEM((3, height * blocks, 128), jnp.float32)],
        compiler_params=pltpu.CompilerParams(vmem_limit_bytes=VMEM_LIMIT),
        name="settle",
    )(tables, got0, got1, got2, got_ghost, jnp.asarray(grow, bf16))
    return out[None]


def solution(mesh):
    placed = (
        P("lvl", None, "blk", None),
        P("lvl", "blk", None),
        P("lvl", "blk"),
        P("lvl", "blk"),
        P("lvl", "blk"),
    )
    step = functools.partial(body, mesh.shape["blk"], mesh.shape["lvl"])
    return jax.shard_map(
        step, mesh=mesh, in_specs=placed, out_specs=P("lvl", None, "blk", None), check_vma=False
    )
```

```python
import functools

import jax
import jax.numpy as jnp
import numpy as np
from jax import lax
from jax.experimental import pallas as pl
from jax.experimental.pallas import tpu as pltpu
from jax.sharding import PartitionSpec as P

MESH = pl.DeviceIdType.MESH
EDGE = 32
PLANE = EDGE * EDGE
HALO = 2 * PLANE
CAP = 2
VMEM_LIMIT = 60 * 1024 * 1024


def device(blk, lvl):
    return {"blk": blk, "lvl": lvl}


def enter(n, levels, me, lvl):
    barrier = pltpu.get_barrier_semaphore()

    def greet(blk, level):
        pl.semaphore_signal(barrier, inc=1, device_id=device(blk, level), device_id_type=MESH)

    for k in range(1, n):
        greet(lax.rem(me + k, n), lvl)

    @pl.when(lvl > 0)
    def _():
        for k in range(n):
            greet(lax.rem(me + k, n), lvl - 1)

    @pl.when(lvl < levels - 1)
    def _():
        for k in range(n):
            greet(lax.rem(me + k, n), lvl + 1)

    pl.semaphore_wait(
        barrier, n - 1 + n * ((lvl > 0).astype(jnp.int32) + (lvl < levels - 1).astype(jnp.int32))
    )


def remote(src, dst, send, recv, target):
    return pltpu.make_async_remote_copy(
        src_ref=src, dst_ref=dst, send_sem=send, recv_sem=recv, device_id=target, device_id_type=MESH
    )


def tap_weights(shifts):
    size = jnp.abs(shifts)
    rest = 1.0 - size
    size2 = size * size
    rest2 = rest * rest
    middle = 1.0 + size2 * (1.5 * size - 2.5)
    ahead = 1.0 + rest2 * (1.5 * rest - 2.5)
    behind = -0.5 * rest2 * size
    far = -0.5 * size2 * rest
    up = shifts >= 0.0
    return {
        -2: jnp.where(up, 0.0, far),
        -1: jnp.where(up, behind, ahead),
        0: middle,
        1: jnp.where(up, ahead, behind),
        2: jnp.where(up, far, 0.0),
    }


def picks(keys, wanted):
    count, first, second = jnp.int32(0), jnp.int32(0), jnp.int32(0)
    for b, key in enumerate(keys):
        hit = key == wanted
        first = jnp.where(jnp.logical_and(hit, count == 0), b, first)
        second = jnp.where(jnp.logical_and(hit, count == 1), b, second)
        count = count + hit.astype(jnp.int32)
    return first, second


def move_kernel(n, levels, spots, parent_slot, flags, vort, shift, shrink,
                got0, got1, got2, got_ghost, tables,
                send0, send1, send2, ghost, below_v, below_s, above_v, above_s, rows, whole, small, local, tab,
                near_s, near_r, coarse_s, coarse_r, halo_s, halo_r, block_s, block_r, ghost_s, ghost_r,
                own_sem, table_sem):
    me = lax.axis_index("blk")
    lvl = lax.axis_index("lvl")
    blocks, cells = vort.shape[1:]
    lane_tiles = PLANE // 128
    height = cells // 128
    quarter = height // 4
    coarse_level = jnp.maximum(lvl - 1, 0)
    got, send = (got0, got1, got2), (send0, send1, send2)
    after = device(lax.rem(me + 1, n), lvl)
    before = device(lax.rem(me + n - 1, n), lvl)
    lane = lax.broadcasted_iota(jnp.int32, (1, 128), 1)
    line = jnp.zeros((1, 128), jnp.int32)
    for part, ref in enumerate((spots, parent_slot, flags)):
        for b in range(blocks):
            line = jnp.where(lane == part * blocks + b, ref[0, b], line)
    tab[...] = line
    enter(n, levels, me, lvl)

    def high(target):
        part = pl.ds(cells - HALO, HALO)
        return (
            remote(vort.at[:, :, part], below_v, halo_s.at[0], halo_r.at[0], target),
            remote(shift.at[:, part], below_s, halo_s.at[1], halo_r.at[1], target),
        )

    def low(target):
        part = pl.ds(0, HALO)
        return (
            remote(vort.at[:, :, part], above_v, halo_s.at[2], halo_r.at[2], target),
            remote(shift.at[:, part], above_s, halo_s.at[3], halo_r.at[3], target),
        )

    def near(k):
        return remote(tab, tables.at[0, me], near_s.at[k], near_r.at[k], device(lax.rem(me + k, n), lvl))

    def coarse(k):
        return remote(tab, tables.at[1, me], coarse_s.at[k], coarse_r.at[k],
                      device(lax.rem(me + k, n), coarse_level))

    @pl.when(me < n - 1)
    def _():
        for copy in high(after):
            copy.start()

    @pl.when(me > 0)
    def _():
        for copy in low(before):
            copy.start()

    for k in range(1, n):
        near(k).start()

    @pl.when(lvl > 0)
    def _():
        for k in range(n):
            coarse(k).start()

    tables[0, me] = tab[...]
    owners = [lax.div(spots[0, b], blocks) for b in range(blocks)]

    sublane = lax.broadcasted_iota(jnp.int32, (blocks, 128), 0)

    def tile(ref, c, at):
        part = ref[c, :, pl.ds(at, 128)] if c is not None else ref[:, pl.ds(at, 128)]
        return part.astype(jnp.float32)

    def source_tile(own, c, x, j):
        at = pl.multiple_of((x % EDGE) * PLANE + j * 128, 128)
        value = tile(own, c, at)
        if x < 0:
            return jnp.where(sublane == 0, 0.0, pltpu.roll(value, 1, 0))
        if x >= EDGE:
            return jnp.where(sublane == blocks - 1, 0.0, pltpu.roll(value, blocks - 1, 0))
        return value

    def outer_tile(below, above, c, x, j):
        if x < 0:
            value = pltpu.roll(tile(below, c, pl.multiple_of((2 + x) * PLANE + j * 128, 128)), 1, 0)
            return jnp.where(jnp.logical_and(sublane == 0, me > 0), value, 0.0)
        value = tile(above, c, pl.multiple_of((x - EDGE) * PLANE + j * 128, 128))
        value = pltpu.roll(value, blocks - 1, 0)
        return jnp.where(jnp.logical_and(sublane == blocks - 1, me < n - 1), value, 0.0)

    def deposit(sums, value, weights, x):
        for offset in range(-2, 3):
            to = x + offset
            if 0 <= to < EDGE:
                term = value * weights[offset]
                sums[to] = sums[to] + term if to in sums else term

    def row_tile(x, j):
        return pl.ds(pl.multiple_of((x * lane_tiles + j) * blocks, blocks), blocks)

    def remesh(c):
        def chunk(j, carry):
            sums = {}
            for x in range(-2, EDGE + 2):
                weights = tap_weights(source_tile(shift, None, x, j))
                deposit(sums, source_tile(vort, c, x, j), weights, x)
                if 0 <= x - 2 < EDGE:
                    rows[row_tile(x - 2, j), :] = sums.pop(x - 2)
            return carry

        lax.fori_loop(0, lane_tiles, chunk, 0)

    def join(c):
        def chunk(j, carry):
            sums = {}
            for x in (-2, -1, EDGE, EDGE + 1):
                weights = tap_weights(outer_tile(below_s, above_s, None, x, j))
                deposit(sums, outer_tile(below_v, above_v, c, x, j), weights, x)
            for x, term in sums.items():
                rows[row_tile(x, j), :] += term
            return carry

        lax.fori_loop(0, lane_tiles, chunk, 0)
        for b in range(blocks):
            whole[b] = rows[pl.ds(b, height, stride=blocks), :].astype(jnp.bfloat16)

    def block_copy(c, k):
        to = lax.rem(me + k, n)
        return remote(send[c].at[to], got[c].at[me], block_s.at[c, k], block_r.at[c, k], device(to, lvl))

    def own_copy(c):
        return pltpu.make_async_copy(send[c].at[me], got[c].at[me], own_sem.at[c])

    def ghost_copy(c, k):
        to = lax.rem(me + k, n)
        return remote(ghost.at[c, to], got_ghost.at[c, me], ghost_s.at[c, k], ghost_r.at[c, k],
                      device(to, coarse_level))

    def send_blocks(c):
        def pack(k, carry):
            to = lax.rem(me + k, n)
            first, second = picks(owners, to)
            send[c][to, 0] = whole[first]
            send[c][to, 1] = whole[second]
            return carry

        lax.fori_loop(1, n + 1, pack, 0)
        for k in range(1, n):
            block_copy(c, k).start()
        own_copy(c).start()

    def restrict(c):
        for b in range(blocks):
            block = whole[b]
            wide = jnp.concatenate([block[q * quarter:(q + 1) * quarter] for q in range(4)], axis=1)
            pairs = jnp.dot(wide, shrink[...], preferred_element_type=jnp.float32)
            pairs = pairs.reshape(4, 2, 8, 128)
            small[c, b] = (pairs[:, 0] + pairs[:, 1]).reshape(32, 128).astype(jnp.bfloat16)

    def send_ghosts(c, parents):
        def pack(k, carry):
            to = lax.rem(me + k, n)
            first, second = picks(parents, to)
            ghost[c, to, 0] = small[c, first]
            ghost[c, to, 1] = small[c, second]
            return carry

        lax.fori_loop(0, n, pack, 0)

        @pl.when(lvl > 0)
        def _():
            for k in range(n):
                ghost_copy(c, k).start()

    remesh(0)

    @pl.when(me < n - 1)
    def _():
        for copy in low(after):
            copy.wait_recv()

    @pl.when(me > 0)
    def _():
        for copy in high(before):
            copy.wait_recv()

    join(0)
    send_blocks(0)

    for k in range(1, n):
        source = lax.rem(me + n - k, n)
        remote(tab, tables.at[0, source], near_s.at[k], near_r.at[k], before).wait_recv()
    fetch = pltpu.make_async_copy(tables.at[0], local, table_sem)
    fetch.start()
    restrict(0)
    fetch.wait()
    parents = []
    for b in range(blocks):
        home, spot = lax.div(spots[0, b], blocks), lax.rem(spots[0, b], blocks)
        parents.append(lax.div(local[home, 0, blocks + spot], 8 * blocks))
    send_ghosts(0, parents)
    remesh(1)
    join(1)
    send_blocks(1)
    restrict(1)
    send_ghosts(1, parents)
    remesh(2)
    join(2)
    restrict(2)
    send_ghosts(2, parents)
    send_blocks(2)

    @pl.when(lvl > 0)
    def _():
        for k in range(n):
            coarse(k).wait_send()
            for c in range(3):
                ghost_copy(c, k).wait_send()

    @pl.when(lvl < levels - 1)
    def _():
        for k in range(n):
            source = lax.rem(me + n - k, n)
            remote(tab, tables.at[1, source], coarse_s.at[k], coarse_r.at[k], before).wait_recv()

    @pl.when(me < n - 1)
    def _():
        for copy in high(after):
            copy.wait_send()

    @pl.when(me > 0)
    def _():
        for copy in low(before):
            copy.wait_send()

    for k in range(1, n):
        near(k).wait_send()
    for c in range(3):
        own_copy(c).wait()
        for k in range(1, n):
            source = lax.rem(me + n - k, n)
            remote(send[c].at[me], got[c].at[source], block_s.at[c, k], block_r.at[c, k], before).wait_recv()
            block_copy(c, k).wait_send()

    @pl.when(lvl < levels - 1)
    def _():
        for c in range(3):
            for k in range(n):
                source = lax.rem(me + n - k, n)
                remote(ghost.at[c, me], got_ghost.at[c, source], ghost_s.at[c, k], ghost_r.at[c, k],
                       before).wait_recv()


def split(value, size):
    if size & (size - 1) == 0:
        return lax.shift_right_logical(value, size.bit_length() - 1), lax.bitwise_and(value, size - 1)
    return lax.div(value, size), lax.rem(value, size)


def settle_kernel(n, levels, tables, got0, got1, got2, got_ghost, grow, out, rows, moved, places, ghosts, sem):
    me = lax.axis_index("blk")
    lvl = lax.axis_index("lvl")
    blocks = out.shape[1]
    height = rows.shape[1] // blocks

    def place(e, count):
        source, b = split(e, blocks)
        count = jnp.where(b == 0, 0, count)
        owner, spot = split(tables[0, source, 0, b], blocks)
        mine = owner == me
        places[jnp.where(mine, spot, blocks)] = source * CAP + count
        return count + mine.astype(jnp.int32)

    lax.fori_loop(0, n * blocks, place, jnp.int32(0), unroll=8)

    def fetch(c, q):
        source, rank = split(places[q], CAP)
        got = (got0, got1, got2)[c]
        return pltpu.make_async_copy(got.at[source, rank], moved.at[c, q], sem.at[c, q])

    for c in range(3):
        for q in range(blocks):
            fetch(c, q).start()

    def seek(e, carry):
        count, total = carry
        source, b = split(e, blocks)
        count = jnp.where(b == 0, 0, count)
        home, spot = split(tables[1, source, 0, b], blocks)
        owner, code = split(tables[1, home, 0, blocks + spot], 8 * blocks)
        mine = owner == me
        ghosts[total] = code * (n * CAP) + source * CAP + count
        hit = jnp.logical_and(mine, tables[1, home, 0, 2 * blocks + spot] == 1)
        return count + mine.astype(jnp.int32), total + hit.astype(jnp.int32)

    rounds = jnp.where(lvl < levels - 1, n, 0)

    def seek_device(source, carry):
        for b in range(blocks):
            carry = seek(source * blocks + b, carry)
        return carry

    total = lax.fori_loop(0, rounds, seek_device, (jnp.int32(0), jnp.int32(0)))[1]

    for c in range(3):
        for q in range(blocks):
            fetch(c, q).wait()
            rows[c, pl.ds(q, height, stride=blocks), :] = moved[c, q].astype(jnp.float32)

    row = lax.broadcasted_iota(jnp.int32, (32, 32), 0)
    column = lax.broadcasted_iota(jnp.int32, (32, 32), 1)
    mask_row = lax.broadcasted_iota(jnp.int32, (32, 128), 0)
    mask_lane = lax.broadcasted_iota(jnp.int32, (32, 128), 1)

    def refine(g, carry):
        code, slot = split(ghosts[g], n * CAP)
        source, rank = split(slot, CAP)
        spot, octant = split(code, 8)
        ox, rest = split(octant, 4)
        oy, oz = split(rest, 2)
        block = jnp.concatenate([got_ghost[c, source, rank] for c in range(3)], axis=1)
        halves = []
        for half in range(2):
            hot = jnp.logical_and(row // 8 == column // 8, column % 8 == 2 * (row % 8 - 4 * oy) + half)
            hot = hot.astype(jnp.float32).astype(jnp.bfloat16)
            halves.append(jnp.dot(hot, block, preferred_element_type=jnp.float32))
        wide = jnp.concatenate(
            [jnp.concatenate([part[:, c * 128:(c + 1) * 128] for part in halves], axis=1) for c in range(3)],
            axis=0,
        ).astype(jnp.bfloat16)
        full = jnp.dot(wide, grow[oz], preferred_element_type=jnp.float32)
        mask = jnp.logical_and(mask_row % 8 // 4 == oy, mask_lane % 32 // 16 == oz)
        for c in range(3):
            for q in range(4):
                spots = pl.ds((ox * 128 + q * 32) * blocks + spot, 32, stride=blocks)
                part = full[c * 32:(c + 1) * 32, q * 128:(q + 1) * 128]
                rows[c, spots, :] = jnp.where(mask, part, rows[c, spots, :])
        return carry

    lax.fori_loop(0, total, refine, 0)

    def finish(r, carry):
        for c in range(3):
            for step in range(8):
                at = r * 8 + step
                out[c, :, pl.ds(pl.multiple_of(at * 128, 128), 128)] = rows[
                    c, pl.ds(pl.multiple_of(at * blocks, blocks), blocks), :
                ].astype(jnp.bfloat16)
        return carry

    lax.fori_loop(0, height // 8, finish, 0)


def selection_tables():
    src = np.arange(512)
    to = np.arange(128)
    q, y, z = src // 128, src % 128 // 32, src % 32
    target = q * 32 + (y // 2) * 16 + z // 2
    shrink = np.where(target[:, None] == to[None, :], 0.125, 0.0)
    part = np.arange(256)
    half, pq, py, pz = part // 128, part % 128 // 32, part % 32 // 16, part % 16
    grow = np.zeros((2, 256, 512))
    for oz in range(2):
        grow[oz, part, pq * 128 + (2 * half + py) * 32 + oz * 16 + pz] = 1.0
    return shrink, grow


def body(n, levels, vorticity, shift_field, new_index, parent_slot, flags):
    blocks, cells = vorticity.shape[2:]
    vort, shift = vorticity[0], shift_field[0]
    any_space = pl.BlockSpec(memory_space=pl.ANY)
    vmem = pl.BlockSpec(memory_space=pltpu.VMEM)
    smem = pl.BlockSpec(memory_space=pltpu.SMEM)
    bf16 = jnp.bfloat16
    shape = jax.ShapeDtypeStruct
    dma = pltpu.SemaphoreType.DMA
    height = cells // 128

    shrink, grow = selection_tables()
    many = shape((n, CAP, height, 128), bf16)
    vm = pltpu.VMEM
    got0, got1, got2, got_ghost, tables = pl.pallas_call(
        functools.partial(move_kernel, n, levels),
        out_shape=(many, many, many, shape((3, n, CAP, 32, 128), bf16), shape((2, n, 1, 128), jnp.int32)),
        in_specs=[smem, smem, smem, vmem, vmem, vmem],
        out_specs=(any_space,) * 4 + (vmem,),
        scratch_shapes=[
            vm(many.shape, bf16), vm(many.shape, bf16), vm(many.shape, bf16),
            vm((3, n, CAP, 32, 128), bf16),
            vm((3, blocks, HALO), bf16), vm((blocks, HALO), bf16),
            vm((3, blocks, HALO), bf16), vm((blocks, HALO), bf16),
            vm((height * blocks, 128), jnp.float32), vm((blocks, height, 128), bf16),
            vm((3, blocks, 32, 128), bf16), pltpu.SMEM((n, 1, 128), jnp.int32),
            vm((1, 128), jnp.int32),
            dma((n,)), dma((n,)), dma((n,)), dma((n,)), dma((4,)), dma((4,)),
            dma((3, n)), dma((3, n)), dma((3, n)), dma((3, n)), dma((3,)), dma,
        ],
        compiler_params=pltpu.CompilerParams(
            collective_id=0, has_side_effects=True, vmem_limit_bytes=VMEM_LIMIT
        ),
        name="move",
    )(new_index, parent_slot, flags, vort, shift, jnp.asarray(shrink, bf16))

    out = pl.pallas_call(
        functools.partial(settle_kernel, n, levels),
        out_shape=shape((3, blocks, cells), bf16),
        in_specs=[smem, any_space, any_space, any_space, vmem, vmem],
        out_specs=vmem,
        scratch_shapes=[
            vm((3, height * blocks, 128), jnp.float32), vm((3, blocks, height, 128), bf16),
            pltpu.SMEM((2 * blocks,), jnp.int32), pltpu.SMEM((n * CAP + 8,), jnp.int32), dma((3, blocks)),
        ],
        compiler_params=pltpu.CompilerParams(vmem_limit_bytes=VMEM_LIMIT),
        name="settle",
    )(tables, got0, got1, got2, got_ghost, jnp.asarray(grow, bf16))
    return out[None]


def solution(mesh):
    placed = (
        P("lvl", None, "blk", None),
        P("lvl", "blk", None),
        P("lvl", "blk"),
        P("lvl", "blk"),
        P("lvl", "blk"),
    )
    step = functools.partial(body, mesh.shape["blk"], mesh.shape["lvl"])
    return jax.shard_map(
        step, mesh=mesh, in_specs=placed, out_specs=P("lvl", None, "blk", None), check_vma=False
    )
```

```python
import functools

import jax
import jax.numpy as jnp
import numpy as np
from jax import lax
from jax.experimental import pallas as pl
from jax.experimental.pallas import tpu as pltpu
from jax.sharding import PartitionSpec as P

MESH = pl.DeviceIdType.MESH
EDGE = 32
PLANE = EDGE * EDGE
HALO = 2 * PLANE
CAP = 2
VMEM_LIMIT = 60 * 1024 * 1024


def device(blk, lvl):
    return {"blk": blk, "lvl": lvl}


def enter(n, levels, me, lvl):
    barrier = pltpu.get_barrier_semaphore()

    def greet(blk, level):
        pl.semaphore_signal(barrier, inc=1, device_id=device(blk, level), device_id_type=MESH)

    for k in range(1, n):
        greet(lax.rem(me + k, n), lvl)

    @pl.when(lvl > 0)
    def _():
        for k in range(n):
            greet(lax.rem(me + k, n), lvl - 1)

    @pl.when(lvl < levels - 1)
    def _():
        for k in range(n):
            greet(lax.rem(me + k, n), lvl + 1)

    pl.semaphore_wait(
        barrier, n - 1 + n * ((lvl > 0).astype(jnp.int32) + (lvl < levels - 1).astype(jnp.int32))
    )


def remote(src, dst, send, recv, target):
    return pltpu.make_async_remote_copy(
        src_ref=src, dst_ref=dst, send_sem=send, recv_sem=recv, device_id=target, device_id_type=MESH
    )


def tap_weights(shifts):
    size = jnp.abs(shifts)
    rest = 1.0 - size
    size2 = size * size
    rest2 = rest * rest
    middle = 1.0 + size2 * (1.5 * size - 2.5)
    ahead = 1.0 + rest2 * (1.5 * rest - 2.5)
    behind = -0.5 * rest2 * size
    far = -0.5 * size2 * rest
    up = shifts >= 0.0
    return {
        -2: jnp.where(up, 0.0, far),
        -1: jnp.where(up, behind, ahead),
        0: middle,
        1: jnp.where(up, ahead, behind),
        2: jnp.where(up, far, 0.0),
    }


def partner(me, k, n):
    if n & (n - 1):
        return lax.rem(me + k, n), lax.rem(me + n - k, n)
    other, bit = 0, 1
    while bit < n:
        other = other + lax.rem(lax.div(me, bit) + k // bit % 2, 2) * bit
        bit *= 2
    return other, other


def picks(keys, wanted):
    count, first, second = jnp.int32(0), jnp.int32(0), jnp.int32(0)
    for b, key in enumerate(keys):
        hit = key == wanted
        first = jnp.where(jnp.logical_and(hit, count == 0), b, first)
        second = jnp.where(jnp.logical_and(hit, count == 1), b, second)
        count = count + hit.astype(jnp.int32)
    return first, second


def move_kernel(n, levels, spots, parent_slot, flags, vort, shift, shrink,
                got0, got1, got2, got_ghost, tables,
                send0, send1, send2, ghost, below_v, below_s, above_v, above_s, rows, whole, small, local, tab,
                near_s, near_r, coarse_s, coarse_r, halo_s, halo_r, block_s, block_r, ghost_s, ghost_r,
                own_sem, table_sem):
    me = lax.axis_index("blk")
    lvl = lax.axis_index("lvl")
    blocks, cells = vort.shape[1:]
    lane_tiles = PLANE // 128
    height = cells // 128
    quarter = height // 4
    coarse_level = jnp.maximum(lvl - 1, 0)
    got, send = (got0, got1, got2), (send0, send1, send2)
    after = device(lax.rem(me + 1, n), lvl)
    before = device(lax.rem(me + n - 1, n), lvl)
    lane = lax.broadcasted_iota(jnp.int32, (1, 128), 1)
    line = jnp.zeros((1, 128), jnp.int32)
    for part, ref in enumerate((spots, parent_slot, flags)):
        for b in range(blocks):
            line = jnp.where(lane == part * blocks + b, ref[0, b], line)
    tab[...] = line
    enter(n, levels, me, lvl)

    def high(target):
        part = pl.ds(cells - HALO, HALO)
        return (
            remote(vort.at[:, :, part], below_v, halo_s.at[0], halo_r.at[0], target),
            remote(shift.at[:, part], below_s, halo_s.at[1], halo_r.at[1], target),
        )

    def low(target):
        part = pl.ds(0, HALO)
        return (
            remote(vort.at[:, :, part], above_v, halo_s.at[2], halo_r.at[2], target),
            remote(shift.at[:, part], above_s, halo_s.at[3], halo_r.at[3], target),
        )

    def near(k):
        return remote(tab, tables.at[0, me], near_s.at[k], near_r.at[k], device(lax.rem(me + k, n), lvl))

    def coarse(k):
        return remote(tab, tables.at[1, me], coarse_s.at[k], coarse_r.at[k],
                      device(lax.rem(me + k, n), coarse_level))

    @pl.when(me < n - 1)
    def _():
        for copy in high(after):
            copy.start()

    @pl.when(me > 0)
    def _():
        for copy in low(before):
            copy.start()

    for k in range(1, n):
        near(k).start()

    @pl.when(lvl > 0)
    def _():
        for k in range(n):
            coarse(k).start()

    tables[0, me] = tab[...]
    owners = [lax.div(spots[0, b], blocks) for b in range(blocks)]

    sublane = lax.broadcasted_iota(jnp.int32, (blocks, 128), 0)

    def tile(ref, c, at):
        part = ref[c, :, pl.ds(at, 128)] if c is not None else ref[:, pl.ds(at, 128)]
        return part.astype(jnp.float32)

    def source_tile(own, c, x, j):
        at = pl.multiple_of((x % EDGE) * PLANE + j * 128, 128)
        value = tile(own, c, at)
        if x < 0:
            return jnp.where(sublane == 0, 0.0, pltpu.roll(value, 1, 0))
        if x >= EDGE:
            return jnp.where(sublane == blocks - 1, 0.0, pltpu.roll(value, blocks - 1, 0))
        return value

    def outer_tile(below, above, c, x, j):
        if x < 0:
            value = pltpu.roll(tile(below, c, pl.multiple_of((2 + x) * PLANE + j * 128, 128)), 1, 0)
            return jnp.where(jnp.logical_and(sublane == 0, me > 0), value, 0.0)
        value = tile(above, c, pl.multiple_of((x - EDGE) * PLANE + j * 128, 128))
        value = pltpu.roll(value, blocks - 1, 0)
        return jnp.where(jnp.logical_and(sublane == blocks - 1, me < n - 1), value, 0.0)

    def deposit(sums, value, weights, x):
        for offset in range(-2, 3):
            to = x + offset
            if 0 <= to < EDGE:
                term = value * weights[offset]
                sums[to] = sums[to] + term if to in sums else term

    def row_tile(x, j):
        return pl.ds(pl.multiple_of((x * lane_tiles + j) * blocks, blocks), blocks)

    def remesh(c):
        def chunk(j, carry):
            sums = {}
            for x in range(-2, EDGE + 2):
                weights = tap_weights(source_tile(shift, None, x, j))
                deposit(sums, source_tile(vort, c, x, j), weights, x)
                if 0 <= x - 2 < EDGE:
                    rows[row_tile(x - 2, j), :] = sums.pop(x - 2)
            return carry

        lax.fori_loop(0, lane_tiles, chunk, 0)

    def join(c):
        def chunk(j, carry):
            sums = {}
            for x in (-2, -1, EDGE, EDGE + 1):
                weights = tap_weights(outer_tile(below_s, above_s, None, x, j))
                deposit(sums, outer_tile(below_v, above_v, c, x, j), weights, x)
            for x, term in sums.items():
                rows[row_tile(x, j), :] += term
            return carry

        lax.fori_loop(0, lane_tiles, chunk, 0)
        for b in range(blocks):
            whole[b] = rows[pl.ds(b, height, stride=blocks), :].astype(jnp.bfloat16)

    def block_copy(c, k):
        to = partner(me, k, n)[0]
        return remote(send[c].at[to], got[c].at[me], block_s.at[c, k], block_r.at[c, k], device(to, lvl))

    def own_copy(c):
        return pltpu.make_async_copy(send[c].at[me], got[c].at[me], own_sem.at[c])

    def ghost_copy(c, k):
        to = partner(me, k, n)[0]
        return remote(ghost.at[c, to], got_ghost.at[c, me], ghost_s.at[c, k], ghost_r.at[c, k],
                      device(to, coarse_level))

    def send_blocks(c):
        def pack(k, carry):
            to = lax.rem(me + k, n)
            first, second = picks(owners, to)
            send[c][to, 0] = whole[first]
            send[c][to, 1] = whole[second]
            return carry

        lax.fori_loop(1, n + 1, pack, 0)
        for k in range(n - 1, 0, -1):
            block_copy(c, k).start()
        own_copy(c).start()

    def restrict(c):
        for b in range(blocks):
            block = whole[b]
            wide = jnp.concatenate([block[q * quarter:(q + 1) * quarter] for q in range(4)], axis=1)
            pairs = jnp.dot(wide, shrink[...], preferred_element_type=jnp.float32)
            pairs = pairs.reshape(4, 2, 8, 128)
            small[c, b] = (pairs[:, 0] + pairs[:, 1]).reshape(32, 128).astype(jnp.bfloat16)

    def send_ghosts(c, parents):
        def pack(k, carry):
            to = lax.rem(me + k, n)
            first, second = picks(parents, to)
            ghost[c, to, 0] = small[c, first]
            ghost[c, to, 1] = small[c, second]
            return carry

        lax.fori_loop(0, n, pack, 0)

        @pl.when(lvl > 0)
        def _():
            for k in range(n - 1, -1, -1):
                ghost_copy(c, k).start()

    remesh(0)

    @pl.when(me < n - 1)
    def _():
        for copy in low(after):
            copy.wait_recv()

    @pl.when(me > 0)
    def _():
        for copy in high(before):
            copy.wait_recv()

    join(0)
    send_blocks(0)

    for k in range(1, n):
        source = lax.rem(me + n - k, n)
        remote(tab, tables.at[0, source], near_s.at[k], near_r.at[k], before).wait_recv()
    fetch = pltpu.make_async_copy(tables.at[0], local, table_sem)
    fetch.start()
    restrict(0)
    fetch.wait()
    parents = []
    for b in range(blocks):
        home, spot = lax.div(spots[0, b], blocks), lax.rem(spots[0, b], blocks)
        parents.append(lax.div(local[home, 0, blocks + spot], 8 * blocks))
    send_ghosts(0, parents)
    remesh(1)
    join(1)
    send_blocks(1)
    restrict(1)
    send_ghosts(1, parents)
    remesh(2)
    join(2)
    restrict(2)
    send_ghosts(2, parents)
    send_blocks(2)

    @pl.when(lvl > 0)
    def _():
        for k in range(n):
            coarse(k).wait_send()
            for c in range(3):
                ghost_copy(c, k).wait_send()

    @pl.when(lvl < levels - 1)
    def _():
        for k in range(n):
            source = lax.rem(me + n - k, n)
            remote(tab, tables.at[1, source], coarse_s.at[k], coarse_r.at[k], before).wait_recv()

    @pl.when(me < n - 1)
    def _():
        for copy in high(after):
            copy.wait_send()

    @pl.when(me > 0)
    def _():
        for copy in low(before):
            copy.wait_send()

    for k in range(1, n):
        near(k).wait_send()
    for c in range(3):
        own_copy(c).wait()
        for k in range(1, n):
            source = partner(me, k, n)[1]
            remote(send[c].at[me], got[c].at[source], block_s.at[c, k], block_r.at[c, k], before).wait_recv()
            block_copy(c, k).wait_send()

    @pl.when(lvl < levels - 1)
    def _():
        for c in range(3):
            for k in range(n):
                source = partner(me, k, n)[1]
                remote(ghost.at[c, me], got_ghost.at[c, source], ghost_s.at[c, k], ghost_r.at[c, k],
                       before).wait_recv()


def split(value, size):
    if size & (size - 1) == 0:
        return lax.shift_right_logical(value, size.bit_length() - 1), lax.bitwise_and(value, size - 1)
    return lax.div(value, size), lax.rem(value, size)


def settle_kernel(n, levels, tables, got0, got1, got2, got_ghost, grow, out, rows, moved, places, ghosts, sem):
    me = lax.axis_index("blk")
    lvl = lax.axis_index("lvl")
    blocks = out.shape[1]
    height = rows.shape[1] // blocks

    def place(e, count):
        source, b = split(e, blocks)
        count = jnp.where(b == 0, 0, count)
        owner, spot = split(tables[0, source, 0, b], blocks)
        mine = owner == me
        places[jnp.where(mine, spot, blocks)] = source * CAP + count
        return count + mine.astype(jnp.int32)

    lax.fori_loop(0, n * blocks, place, jnp.int32(0), unroll=8)

    def fetch(c, q):
        source, rank = split(places[q], CAP)
        got = (got0, got1, got2)[c]
        return pltpu.make_async_copy(got.at[source, rank], moved.at[c, q], sem.at[c, q])

    for c in range(3):
        for q in range(blocks):
            fetch(c, q).start()

    def seek(e, carry):
        count, total = carry
        source, b = split(e, blocks)
        count = jnp.where(b == 0, 0, count)
        home, spot = split(tables[1, source, 0, b], blocks)
        owner, code = split(tables[1, home, 0, blocks + spot], 8 * blocks)
        mine = owner == me
        ghosts[total] = code * (n * CAP) + source * CAP + count
        hit = jnp.logical_and(mine, tables[1, home, 0, 2 * blocks + spot] == 1)
        return count + mine.astype(jnp.int32), total + hit.astype(jnp.int32)

    rounds = jnp.where(lvl < levels - 1, n, 0)

    def seek_device(source, carry):
        for b in range(blocks):
            carry = seek(source * blocks + b, carry)
        return carry

    total = lax.fori_loop(0, rounds, seek_device, (jnp.int32(0), jnp.int32(0)))[1]

    for c in range(3):
        for q in range(blocks):
            fetch(c, q).wait()
            rows[c, pl.ds(q, height, stride=blocks), :] = moved[c, q].astype(jnp.float32)

    row = lax.broadcasted_iota(jnp.int32, (32, 32), 0)
    column = lax.broadcasted_iota(jnp.int32, (32, 32), 1)
    mask_row = lax.broadcasted_iota(jnp.int32, (32, 128), 0)
    mask_lane = lax.broadcasted_iota(jnp.int32, (32, 128), 1)

    def refine(g, carry):
        code, slot = split(ghosts[g], n * CAP)
        source, rank = split(slot, CAP)
        spot, octant = split(code, 8)
        ox, rest = split(octant, 4)
        oy, oz = split(rest, 2)
        block = jnp.concatenate([got_ghost[c, source, rank] for c in range(3)], axis=1)
        halves = []
        for half in range(2):
            hot = jnp.logical_and(row // 8 == column // 8, column % 8 == 2 * (row % 8 - 4 * oy) + half)
            hot = hot.astype(jnp.float32).astype(jnp.bfloat16)
            halves.append(jnp.dot(hot, block, preferred_element_type=jnp.float32))
        wide = jnp.concatenate(
            [jnp.concatenate([part[:, c * 128:(c + 1) * 128] for part in halves], axis=1) for c in range(3)],
            axis=0,
        ).astype(jnp.bfloat16)
        full = jnp.dot(wide, grow[oz], preferred_element_type=jnp.float32)
        mask = jnp.logical_and(mask_row % 8 // 4 == oy, mask_lane % 32 // 16 == oz)
        for c in range(3):
            for q in range(4):
                spots = pl.ds((ox * 128 + q * 32) * blocks + spot, 32, stride=blocks)
                part = full[c * 32:(c + 1) * 32, q * 128:(q + 1) * 128]
                rows[c, spots, :] = jnp.where(mask, part, rows[c, spots, :])
        return carry

    lax.fori_loop(0, total, refine, 0)

    def finish(r, carry):
        for c in range(3):
            for step in range(8):
                at = r * 8 + step
                out[c, :, pl.ds(pl.multiple_of(at * 128, 128), 128)] = rows[
                    c, pl.ds(pl.multiple_of(at * blocks, blocks), blocks), :
                ].astype(jnp.bfloat16)
        return carry

    lax.fori_loop(0, height // 8, finish, 0)


def selection_tables():
    src = np.arange(512)
    to = np.arange(128)
    q, y, z = src // 128, src % 128 // 32, src % 32
    target = q * 32 + (y // 2) * 16 + z // 2
    shrink = np.where(target[:, None] == to[None, :], 0.125, 0.0)
    part = np.arange(256)
    half, pq, py, pz = part // 128, part % 128 // 32, part % 32 // 16, part % 16
    grow = np.zeros((2, 256, 512))
    for oz in range(2):
        grow[oz, part, pq * 128 + (2 * half + py) * 32 + oz * 16 + pz] = 1.0
    return shrink, grow


def body(n, levels, vorticity, shift_field, new_index, parent_slot, flags):
    blocks, cells = vorticity.shape[2:]
    vort, shift = vorticity[0], shift_field[0]
    any_space = pl.BlockSpec(memory_space=pl.ANY)
    vmem = pl.BlockSpec(memory_space=pltpu.VMEM)
    smem = pl.BlockSpec(memory_space=pltpu.SMEM)
    bf16 = jnp.bfloat16
    shape = jax.ShapeDtypeStruct
    dma = pltpu.SemaphoreType.DMA
    height = cells // 128

    shrink, grow = selection_tables()
    many = shape((n, CAP, height, 128), bf16)
    vm = pltpu.VMEM
    got0, got1, got2, got_ghost, tables = pl.pallas_call(
        functools.partial(move_kernel, n, levels),
        out_shape=(many, many, many, shape((3, n, CAP, 32, 128), bf16), shape((2, n, 1, 128), jnp.int32)),
        in_specs=[smem, smem, smem, vmem, vmem, vmem],
        out_specs=(any_space,) * 4 + (vmem,),
        scratch_shapes=[
            vm(many.shape, bf16), vm(many.shape, bf16), vm(many.shape, bf16),
            vm((3, n, CAP, 32, 128), bf16),
            vm((3, blocks, HALO), bf16), vm((blocks, HALO), bf16),
            vm((3, blocks, HALO), bf16), vm((blocks, HALO), bf16),
            vm((height * blocks, 128), jnp.float32), vm((blocks, height, 128), bf16),
            vm((3, blocks, 32, 128), bf16), pltpu.SMEM((n, 1, 128), jnp.int32),
            vm((1, 128), jnp.int32),
            dma((n,)), dma((n,)), dma((n,)), dma((n,)), dma((4,)), dma((4,)),
            dma((3, n)), dma((3, n)), dma((3, n)), dma((3, n)), dma((3,)), dma,
        ],
        compiler_params=pltpu.CompilerParams(
            collective_id=0, has_side_effects=True, vmem_limit_bytes=VMEM_LIMIT
        ),
        name="move",
    )(new_index, parent_slot, flags, vort, shift, jnp.asarray(shrink, bf16))

    out = pl.pallas_call(
        functools.partial(settle_kernel, n, levels),
        out_shape=shape((3, blocks, cells), bf16),
        in_specs=[smem, any_space, any_space, any_space, vmem, vmem],
        out_specs=vmem,
        scratch_shapes=[
            vm((3, height * blocks, 128), jnp.float32), vm((3, blocks, height, 128), bf16),
            pltpu.SMEM((2 * blocks,), jnp.int32), pltpu.SMEM((n * CAP + 8,), jnp.int32), dma((3, blocks)),
        ],
        compiler_params=pltpu.CompilerParams(vmem_limit_bytes=VMEM_LIMIT),
        name="settle",
    )(tables, got0, got1, got2, got_ghost, jnp.asarray(grow, bf16))
    return out[None]


def solution(mesh):
    placed = (
        P("lvl", None, "blk", None),
        P("lvl", "blk", None),
        P("lvl", "blk"),
        P("lvl", "blk"),
        P("lvl", "blk"),
    )
    step = functools.partial(body, mesh.shape["blk"], mesh.shape["lvl"])
    return jax.shard_map(
        step, mesh=mesh, in_specs=placed, out_specs=P("lvl", None, "blk", None), check_vma=False
    )
```
